256 devices in a mesh: row: 8 (over z_lo, x), col: 32 (over y, z_hi, core).
Axes of the slice: x: 4, y: 4, z: 8 (z_hi: 4, z_lo: 2; z = z_hi * 2 + z_lo), core: 2. Of those that a mesh axis runs over, the one named last changes fastest.
Arguments:
- matrix: bfloat16 [4096, 131072], P('row', 'col'), may hold values from -0.09375 to 0.09375
- measured: float32 [256, 4096], P(None, 'row'), may hold values from -160 to 160
- support: int32 [4, 2048], replicated, may hold values from 0 to 131071, as said below
Outputs:
- estimate: float32 [256, 131072], P('row', 'col')
- row_norms: float32 [131072], P('col')
- residual_energy: float32 [4], replicated
The draws below stay inside these ranges and needn't reach their ends.
Inputs may be any that keep to these rules, and one draw needn't show every extreme that they name: Each row of support lists 2048 distinct signal-row indices in increasing order; in every row, each aligned block of 4096 indices (the signal rows of one index of col) holds at most 128 of them, and some block exactly 128.
All inputs are finite; a program needn't handle non-finite values.
Results may differ from the reference program's by a relative error of at most 0.015.
Values may be sent and summed in bfloat16 or wider, within the bound.
No kernel may reach another device: no remote copies, remote signals or barrier semaphores. Data moves between devices by JAX's collectives and lax.ppermute only.
A program may use at most 64 MiB of HBM per device.

```python
import math
import jax
import jax.numpy as jnp
from jax import lax

MB = 512
NB = 4096
L = 256
KB = 64
ITERS = 4
M = 4096
N = 131072
K = 2048
N_ROW = 8
N_COL = 32


def draw_measured(key, part):
    key_base, key_rows, key_signals = jax.random.split(key, 3)
    position = jnp.arange(M, dtype=jnp.float32) / max(M - 1, 1)
    rising = math.log(3.0)
    values = jax.random.normal(key_base, (L, M), jnp.float32)
    values = jnp.clip(values, -5.0, 5.0)
    row_scale = jnp.exp(rising * position + jax.random.uniform(key_rows, (M,), jnp.float32) * math.log(10.0 / 3.0)) / 3.0
    signal_scale = jnp.exp(jax.random.uniform(key_signals, (L,), jnp.float32) * math.log(10.0)) / math.sqrt(10.0)
    return values * row_scale[None, :] * signal_scale[:, None]


def draw_support(key, part):
    blocks = N // NB

    def one_iteration(iteration_key):
        key_order, key_shift, key_ranks = jax.random.split(iteration_key, 3)
        block_order = jax.random.permutation(key_order, blocks)
        shifts = jax.random.randint(key_shift, (blocks // 2,), 0, KB + 1).at[0].set(KB)
        counts = jnp.zeros((blocks,), jnp.int32).at[block_order[0::2]].set(KB + shifts).at[block_order[1::2]].set(KB - shifts)
        rank_table = jax.vmap(lambda block_key: jax.random.permutation(block_key, NB))(jax.random.split(key_ranks, blocks))
        chosen = (rank_table < counts[:, None]).reshape(-1)
        return jnp.nonzero(chosen, size=K)[0].astype(jnp.int32)
    return jax.vmap(one_iteration)(jax.random.split(key, ITERS))


def shard_levels(key, extent, cuts, least, largest):
    factor_of = 1.0
    for dim, shards_of in cuts:
        steps = jax.random.uniform(jax.random.fold_in(jax.random.fold_in(key, 6), dim), (shards_of,), jnp.float32, least / len(cuts), largest / len(cuts))
        factor_of = factor_of * jnp.repeat(jnp.exp(steps), extent[dim] // shards_of).reshape((-1,) + (1,) * (len(extent) - 1 - dim))
    return factor_of


def scatter_about(own_key, extent, deviation, bound, cuts=(), kind=jnp.bfloat16):
    result = deviation * jax.random.normal(own_key, extent, jnp.float32)
    if cuts:
        result = result * shard_levels(own_key, extent, cuts, -0.22, 0.18)
    return jnp.clip(result, -bound, bound).astype(kind)


def setup_inputs(seed: int = 0) -> dict:
    key_of = jax.random.split(jax.random.key(seed), 4)
    return {
        "matrix": scatter_about(key_of[0], (M, N), M ** -0.5, 0.09375, ((0, 8), (1, 32))),
        "measured": draw_measured(jax.random.fold_in(key_of[3], 71), 0),
        "support": draw_support(jax.random.fold_in(key_of[3], 71), 0),
    }


STEP_SIZE = 0.25

def predict(matrix, current_half):

    def add_block(block, summed):
        start_col = (block * NB).astype(jnp.int32)
        columns = lax.dynamic_slice_in_dim(matrix, start_col, NB, 1)
        signal_cols = lax.dynamic_slice_in_dim(current_half, start_col, NB, 1)
        return summed + lax.dot_general(signal_cols, columns, (((1,), (1,)), ((), ())), preferred_element_type=jnp.float32)
    return lax.fori_loop(0, N_COL, add_block, jnp.zeros((L, MB * N_ROW), jnp.float32))

def descend(matrix, residual_half):

    def one_block(block):
        start_col = (block * NB).astype(jnp.int32)
        columns = lax.dynamic_slice_in_dim(matrix, start_col, NB, 1)
        summed = jnp.zeros((L, NB), jnp.float32)
        for group_index in range(N_ROW):
            part_sum = jnp.dot(residual_half[:, group_index * MB:(group_index + 1) * MB], columns[group_index * MB:(group_index + 1) * MB], preferred_element_type=jnp.float32)
            rounded = lax.optimization_barrier(part_sum.astype(jnp.bfloat16))
            summed = summed + rounded.astype(jnp.float32)
        return summed
    blocks_out = lax.map(one_block, jnp.arange(N_COL, dtype=jnp.int32))
    return jnp.transpose(blocks_out, (1, 0, 2)).reshape(L, N_COL * NB)

def reference(matrix, measured, support):
    total_cols = NB * N_COL
    current = jnp.zeros((L, total_cols), jnp.float32)
    energies = []
    stepped = current
    for iteration in range(ITERS):
        if iteration == 0:
            residual = measured
        else:
            residual = measured - predict(matrix, current.astype(jnp.bfloat16))
        energies.append(jnp.sum(residual * residual) / (L * MB * N_ROW))
        gradient = descend(matrix, residual.astype(jnp.bfloat16))
        stepped = current + STEP_SIZE * gradient
        keep_mask = jnp.zeros((total_cols,), jnp.float32).at[support[iteration]].set(1.0)
        current = stepped * keep_mask[None, :]
    row_norms = jnp.sqrt(lax.optimization_barrier(jnp.sum(stepped * stepped, axis=0)))
    return (current, row_norms, jnp.stack(energies))
```

```python
import jax
import jax.numpy as jnp
from jax import lax
from jax.sharding import Mesh
from jax.sharding import PartitionSpec as P

KMAX = 128
STEP_SIZE = 0.25
ROW = ("zl", "x")
COL = ("y", "zh", "c")
SIZES = {"zl": 2, "x": 4, "y": 4, "zh": 4, "c": 2}
HALF = jnp.bfloat16
FULL = jnp.float32


def swap(value, axis, step):
    return lax.ppermute(value, axis, [(i, i ^ step) for i in range(SIZES[axis])])


def take(array, index):
    return lax.dynamic_index_in_dim(array, index, 0, keepdims=False)


def partners(axis):
    return range(1, SIZES[axis])


def spread(tiles, axis):
    me = lax.axis_index(axis)
    arrived = [swap(take(tiles, me ^ s), axis, s) for s in partners(axis)]
    return [take(tiles, me), *arrived]


def gathered(value, axis):
    return [value, *(swap(value, axis, s) for s in partners(axis))]


def summed(parts):
    parts = [p.astype(FULL) for p in parts]
    if len(parts) == 2:
        return parts[0] + parts[1]
    return (parts[0] + parts[1]) + (parts[2] + parts[3])


def absolute(parts, axis):
    me = lax.axis_index(axis)
    stacked = jnp.stack(parts)
    return [take(stacked, me ^ k) for k in range(SIZES[axis])]


def dot(a, b):
    return jnp.dot(a, b, preferred_element_type=FULL)


def dot_t(a, b):
    return lax.dot_general(a, b, (((1,), (1,)), ((), ())), preferred_element_type=FULL)


def exact_dot(a, b):
    return jnp.dot(a, b, precision=lax.Precision.HIGHEST, preferred_element_type=FULL)


def window(padded, below, inside, row):
    kept = lax.dynamic_slice(padded, (row, below), (1, KMAX))[0]
    return jnp.where(jnp.arange(KMAX) < inside, kept, -1)


def same(before, after):
    return ((before[:, None] == after[None, :]) & (before[:, None] >= 0)).astype(FULL)


def local(matrix, measured, support):
    signals, rows = measured.shape
    columns = matrix.shape[1]
    zl, x, y, zh, c = (lax.axis_index(a) for a in (*ROW, *COL))
    group = signals // 8
    few = group // 4
    part = signals // 16
    half_rows = rows // 2

    starts = jnp.stack([((y * 4 + (zh ^ s)) * 2 + c) * columns for s in range(4)])
    below = jnp.sum((support[:, None, :] < starts[None, :, None]).astype(jnp.int32), axis=2)
    until = jnp.sum(
        (support[:, None, :] < starts[None, :, None] + columns).astype(jnp.int32), axis=2
    )
    inside = until - below
    padded = jnp.pad(support, ((0, 0), (0, KMAX)))

    def kept(t, s):
        return window(padded, below[t, s], inside[t, s], t)

    own = [kept(t, 0) for t in range(4)]
    local_index = [jnp.where(k >= 0, k - starts[0], -1) for k in own]
    picked = jnp.concatenate(local_index[:3])
    chosen = (jnp.arange(columns)[:, None] == picked[None, :]).astype(HALF)
    kept_matrix = dot(matrix, chosen).astype(HALF)
    a0, a1, a2 = (kept_matrix[:, KMAX * t : KMAX * (t + 1)] for t in range(3))

    gradient = dot(measured.astype(HALF), a0).astype(HALF)
    tiles = jnp.moveaxis(gradient.reshape(2, 4, group, KMAX), 1, 0).reshape(4, 2 * group, KMAX)
    first = summed(spread(tiles, "x")).astype(HALF)
    current = STEP_SIZE * summed([first, swap(first, "zl", 1)])
    a0_rows = jnp.concatenate(gathered(a0, "x"), axis=0)

    def rows_of(a):
        wide = jnp.concatenate(gathered(a, "zh"), axis=1)
        return jnp.concatenate(gathered(wide, "x"), axis=0)

    a1_all = rows_of(a1)
    a2_all = rows_of(a2)

    mine = take(
        jnp.moveaxis(
            take(jnp.moveaxis(measured.reshape(2, 4, 4, few, rows), 2, 0), zh).reshape(
                2, 4, few, 2, half_rows
            ),
            3,
            0,
        ),
        c,
    )
    mine = jnp.moveaxis(mine, 1, 0).reshape(4, part, half_rows)
    target = jnp.stack(spread(mine, "x"), axis=1)

    def residual_of(image):
        halves = jnp.moveaxis(image.reshape(part, 4, 2, half_rows), 2, 0)
        sent = take(halves, 1 - c).astype(HALF)
        pair = (take(halves, c) + swap(sent, "c", 1).astype(FULL)).astype(HALF)
        return target - summed(gathered(pair, "y"))

    def both_halves(piece, axis):
        other = swap(piece, "c", 1)
        return jnp.stack(
            [jnp.where(c == 0, piece, other), jnp.where(c == 0, other, piece)], axis=axis
        )

    def whole_rows(residual):
        return both_halves(residual.astype(HALF), 2).reshape(part, 4 * rows)

    image = dot_t(current.astype(HALF), a0_rows).astype(HALF)
    image = jnp.moveaxis(image.reshape(2, 4, few, 4 * rows), 1, 0).reshape(4, part, 4 * rows)
    residual = residual_of(summed(spread(image, "zh")))
    energies = [jnp.sum(residual * residual)]

    carried = exact_dot(current, same(own[0], own[1]))
    carried = jnp.moveaxis(carried.reshape(2, 4, few, KMAX), 1, 0).reshape(4, part, KMAX)
    carried = jnp.concatenate(spread(carried, "zh"), axis=1)

    around = [jnp.concatenate([kept(t, s) for s in range(4)]) for t in (1, 2)]

    def step(carried, residual, a):
        partial = dot(whole_rows(residual), a).astype(HALF)
        return carried + STEP_SIZE * summed([partial, swap(partial, "zl", 1)])

    current = step(carried, residual, a1_all)
    residual = residual_of(dot_t(current.astype(HALF), a1_all))
    energies.append(jnp.sum(residual * residual))
    carried = exact_dot(current, same(around[0], around[1]))
    current = step(carried, residual, a2_all)
    residual = residual_of(dot_t(current.astype(HALF), a2_all))
    energies.append(jnp.sum(residual * residual))

    half = jnp.moveaxis(residual.astype(HALF), 1, 0)
    by_x = jnp.stack([half[0], *(swap(half[s], "x", s) for s in partners("x"))])
    by_zh = gathered(by_x, "zh")
    ordered = jnp.stack([jnp.stack(absolute(list(p), "x")) for p in absolute(by_zh, "zh")])
    ordered = both_halves(ordered.reshape(4, 4, 2, few, half_rows), 4)
    ordered = jnp.transpose(ordered, (2, 1, 0, 3, 4, 5)).reshape(signals, rows)

    gradient = dot(ordered, matrix).astype(HALF).reshape(8, group, columns)
    gradient = lax.all_to_all(gradient, ROW, 0, 0, tiled=True).astype(FULL).sum(axis=0)

    blocks = jnp.moveaxis(current.reshape(part, 4, KMAX), 1, 0)
    home = absolute([blocks[0], *(swap(blocks[s], "zh", s) for s in partners("zh"))], "zh")
    home = take(jnp.moveaxis(jnp.stack(home).reshape(4, 2, few, KMAX), 1, 0), zl)
    place = (local_index[2][:, None] == jnp.arange(columns)[None, :]).astype(FULL)
    stepped = exact_dot(home.reshape(group, KMAX), place) + STEP_SIZE * gradient
    keep = jnp.any(local_index[3][:, None] == jnp.arange(columns)[None, :], axis=0)
    estimate = jnp.where(keep[None, :], stepped, 0.0)

    energy = jnp.stack(energies)
    energy = summed([energy, swap(energy, "c", 1)])
    energy = summed(gathered(energy, "zh"))
    vector = jnp.concatenate(
        [jnp.sum(stepped * stepped, axis=0), jnp.sum(measured * measured)[None], energy]
    )
    vector = summed([vector, swap(vector, "zl", 1)])
    vector = summed(gathered(vector, "x"))
    total_count = signals * rows * 8
    return estimate, jnp.sqrt(vector[:columns]), vector[columns:] / total_count


def solution(mesh):
    torus = Mesh(mesh.devices.reshape(2, 4, 4, 4, 2), (*ROW, *COL))
    return jax.shard_map(
        local,
        mesh=torus,
        in_specs=(P(ROW, COL), P(None, ROW), P()),
        out_specs=(P(ROW, COL), P(COL), P()),
        check_vma=False,
    )
```

```python
import jax
import jax.numpy as jnp
from jax import lax
from jax.experimental import pallas as pl
from jax.experimental.pallas import tpu as pltpu
from jax.sharding import Mesh
from jax.sharding import PartitionSpec as P

KMAX = 128
STEPS = 3
STEP_SIZE = 0.25
ROW = ("zl", "x")
COL = ("y", "zh", "c")
SIZES = {"zl": 2, "x": 4, "y": 4, "zh": 4, "c": 2}
HALF = jnp.bfloat16
FULL = jnp.float32
TILE = 1024
BEYOND = 1 << 30


def swap(value, axis, step):
    return lax.ppermute(value, axis, [(i, i ^ step) for i in range(SIZES[axis])])


def take(array, index):
    return lax.dynamic_index_in_dim(array, index, 0, keepdims=False)


def partners(axis):
    return range(1, SIZES[axis])


def spread(tiles, axis):
    me = lax.axis_index(axis)
    arrived = [swap(take(tiles, me ^ s), axis, s) for s in partners(axis)]
    return [take(tiles, me), *arrived]


def gathered(value, axis):
    return [value, *(swap(value, axis, s) for s in partners(axis))]


def summed(parts):
    parts = [p.astype(FULL) for p in parts]
    return (parts[0] + parts[1]) + (parts[2] + parts[3])


def everyone(value):
    copies = jnp.broadcast_to(value, (8, *value.shape))
    return lax.all_to_all(copies, ROW, 0, 0, tiled=True)


def dot(a, b):
    return jnp.dot(a, b, preferred_element_type=FULL)


def dot_t(a, b):
    return lax.dot_general(a, b, (((1,), (1,)), ((), ())), preferred_element_type=FULL)


def rounded(value):
    return lax.reduce_precision(value, 8, 7)


def prepare_body(start_ref, support_ref, measured_ref, matrix_ref, kept_ref, slope_ref, index_ref, total):
    tile = pl.program_id(0)
    start = start_ref[0]
    columns = TILE * pl.num_programs(0)

    @pl.when(tile == 0)
    def _():
        total[...] = jnp.zeros_like(total)
        lane = lax.broadcasted_iota(jnp.int32, (8, KMAX), 1)
        for t in range(STEPS + 1):
            row = support_ref[t : t + 1, :]
            below = jnp.sum((row < start).astype(FULL)).astype(jnp.int32)
            first = pl.multiple_of((below // KMAX) * KMAX, KMAX)
            near = support_ref[:, pl.ds(first, 2 * KMAX)]
            near = pltpu.roll(near, 2 * KMAX - (below - first), 1)[:, :KMAX] - start
            index_ref[t : t + 1, :] = jnp.where(near < columns, near, -1)[t : t + 1, :]
        index_ref[STEPS + 1 :, :] = jnp.full((8 - STEPS - 1, KMAX), -1, jnp.int32)

    picked = jnp.concatenate([index_ref[t : t + 1, :] for t in range(STEPS)], axis=1)
    place = lax.broadcasted_iota(jnp.int32, (TILE, STEPS * KMAX), 0) + tile * TILE
    chosen = jnp.where(place == picked, 1.0, 0.0).astype(HALF)
    total[...] += dot(matrix_ref[...], chosen)

    @pl.when(tile == pl.num_programs(0) - 1)
    def _():
        slope_ref[...] = dot(
            measured_ref[...].astype(HALF), total[:, :KMAX].astype(HALF)
        ).astype(HALF)
        kept_ref[...] = total[...].T.astype(HALF)


def prepare(start, support, measured, matrix):
    signals, rows = measured.shape
    columns = matrix.shape[1]
    padded = jnp.pad(support, ((0, 8 - support.shape[0]), (0, 2 * KMAX)), constant_values=BEYOND)
    return pl.pallas_call(
        prepare_body,
        grid=(columns // TILE,),
        in_specs=[
            pl.BlockSpec(memory_space=pltpu.SMEM),
            pl.BlockSpec(padded.shape, lambda k: (0, 0)),
            pl.BlockSpec(measured.shape, lambda k: (0, 0)),
            pl.BlockSpec((rows, TILE), lambda k: (0, k)),
        ],
        out_specs=[
            pl.BlockSpec((STEPS * KMAX, rows), lambda k: (0, 0)),
            pl.BlockSpec((signals, KMAX), lambda k: (0, 0)),
            pl.BlockSpec((8, KMAX), lambda k: (0, 0)),
        ],
        out_shape=[
            jax.ShapeDtypeStruct((STEPS * KMAX, rows), HALF),
            jax.ShapeDtypeStruct((signals, KMAX), HALF),
            jax.ShapeDtypeStruct((8, KMAX), jnp.int32),
        ],
        scratch_shapes=[pltpu.VMEM((rows, STEPS * KMAX), FULL)],
        cost_estimate=pl.CostEstimate(
            flops=2 * rows * columns * STEPS * KMAX, bytes_accessed=2 * rows * columns, transcendentals=0
        ),
    )(start[None], padded, measured, matrix)


def local(matrix, measured, support):
    signals, rows = measured.shape
    columns = matrix.shape[1]
    zl, x, y, zh, c = (lax.axis_index(a) for a in (*ROW, *COL))
    few = signals // 8
    wide = 8 * KMAX
    kept, slope, index = prepare(((y * 4 + zh) * 2 + c) * columns, support, measured, matrix)

    mine = jnp.stack(spread(slope.reshape(4, 2 * few, KMAX), "y")).reshape(4, 2, few, KMAX)
    mine = jnp.moveaxis(mine, 1, 0)
    pair = jnp.stack([take(mine, c), swap(take(mine, 1 - c), "c", 1)])
    partial = jnp.transpose(pair.reshape(8, few, KMAX), (1, 0, 2)).reshape(few, wide)

    index_rows = jnp.pad(
        jnp.concatenate([index[:STEPS] >> 6, index[:STEPS] & 63], axis=1).astype(HALF),
        ((0, 16 - STEPS), (0, rows - 2 * KMAX)),
    )
    near = jnp.stack(gathered(jnp.concatenate([kept, index_rows]), "y"))
    far = swap(near, "c", 1)
    bases = [
        jnp.concatenate([p[:, t * KMAX : (t + 1) * KMAX] for p in (near, far)]).reshape(wide, rows)
        for t in range(STEPS)
    ]
    codes = jnp.concatenate([p[:, STEPS * KMAX :] for p in (near, far)]).astype(FULL)
    codes = codes[:, :, :KMAX] * 64 + codes[:, :, KMAX : 2 * KMAX]

    target = take(measured.reshape(8, few, rows), y * 2 + c)

    def carry(current, t):
        same = (codes[:, t - 1, :, None] == codes[:, t, None, :]) & (codes[:, t - 1, :, None] >= 0)
        high = rounded(current)
        low = current - high
        values = jnp.concatenate([high, low]).astype(HALF).reshape(2 * few, 8, KMAX)
        moved = lax.dot_general(
            values, same.astype(HALF), (((2,), (1,)), ((1,), (0,))), preferred_element_type=FULL
        )
        moved = jnp.transpose(moved[:, :few] + moved[:, few:], (1, 0, 2))
        return moved.reshape(few, wide)

    current = None
    residual = target
    energies = [jnp.sum(residual * residual)]
    for t in range(STEPS):
        gradient = jnp.sum(everyone(partial).astype(FULL), axis=0)
        stepped = STEP_SIZE * gradient
        current = stepped if t == 0 else carry(current, t) + stepped
        image = dot(current.astype(HALF), bases[t]).astype(HALF)
        residual = target - summed(gathered(image, "zh"))
        energies.append(jnp.sum(residual * residual))
        if t + 1 < STEPS:
            partial = dot_t(residual.astype(HALF), bases[t + 1]).astype(HALF)

    lane = lax.broadcasted_iota(jnp.int32, (few, KMAX), 1)
    first = lax.broadcasted_iota(jnp.int32, (few, KMAX), 0) == 0
    note = jnp.zeros((few, KMAX), FULL)
    for t, energy in enumerate(energies):
        high = rounded(energy)
        middle = rounded(energy - high)
        for k, term in enumerate((high, middle, energy - high - middle)):
            note = jnp.where(first & (lane == 4 * k + t), term, note)
    note = note.astype(HALF)
    residual = residual.astype(HALF)
    blocks = current.astype(HALF)
    one = jnp.concatenate([residual, note, blocks[:, : wide // 2]], axis=1)
    other = swap(jnp.concatenate([residual, note, blocks[:, wide // 2 :]], axis=1), "c", 1)
    both = jnp.concatenate([jnp.where(c == 0, one, other), jnp.where(c == 0, other, one)])
    fixed = both[:, : rows + KMAX]
    ours = [both[:, rows + (1 + s) * KMAX : rows + (2 + s) * KMAX] for s in range(4)]
    packets = [jnp.concatenate([fixed, block], axis=1) for block in ours]
    arrived = jnp.stack([packets[0], *(swap(packets[s], "y", s) for s in partners("y"))])
    ordered = jnp.concatenate([take(arrived, y ^ k) for k in range(4)])

    gradient = dot(ordered[:, :rows], matrix).astype(HALF).reshape(8, few, columns)
    gradient = lax.all_to_all(gradient, ROW, 0, 0, tiled=True).astype(FULL).sum(axis=0)
    home = take(ordered[:, rows + KMAX :].reshape(8, few, KMAX), zl * 4 + x)
    place = jnp.arange(columns)[:, None]
    stepped = dot_t(home, (place == index[2][None, :]).astype(HALF)) + STEP_SIZE * gradient
    keep = jnp.any(index[3][:, None] == jnp.arange(columns)[None, :], axis=0)
    estimate = jnp.where(keep[None, :], stepped, 0.0)

    squares = jnp.sum(stepped * stepped, axis=0).reshape(columns // KMAX, KMAX)
    notes = jnp.sum(ordered[:, rows : rows + KMAX].astype(FULL), axis=0, keepdims=True)
    totals = jnp.concatenate([squares, jnp.pad(notes, ((0, 7), (0, 0)))])
    totals = jnp.sum(everyone(totals), axis=0)
    energy = totals[columns // KMAX, :12].reshape(3, 4).sum(axis=0)
    return (
        estimate,
        jnp.sqrt(totals[: columns // KMAX]).reshape(columns),
        energy / (signals * rows * 8),
    )


def solution(mesh):
    torus = Mesh(mesh.devices.reshape(2, 4, 4, 4, 2), (*ROW, *COL))
    return jax.shard_map(
        local,
        mesh=torus,
        in_specs=(P(ROW, COL), P(None, ROW), P()),
        out_specs=(P(ROW, COL), P(COL), P()),
        check_vma=False,
    )
```

```python
import jax
import jax.numpy as jnp
from jax import lax
from jax.experimental import pallas as pl
from jax.experimental.pallas import tpu as pltpu
from jax.sharding import Mesh
from jax.sharding import PartitionSpec as P

KMAX = 128
STEPS = 3
STEP_SIZE = 0.25
ROW = ("zl", "x")
COL = ("y", "zh", "c")
SIZES = {"zl": 2, "x": 4, "y": 4, "zh": 4, "c": 2}
HALF = jnp.bfloat16
FULL = jnp.float32
TILE = 1024


def swap(value, axis, step):
    return lax.ppermute(value, axis, [(i, i ^ step) for i in range(SIZES[axis])])


def take(array, index):
    return lax.dynamic_index_in_dim(array, index, 0, keepdims=False)


def partners(axis):
    return range(1, SIZES[axis])


def swaps(value_for, axis):
    arrived = [value_for(0)]
    for s in partners(axis):
        arrived.append(swap(value_for(s), axis, s))
    return arrived


def spread(tiles, axis):
    me = lax.axis_index(axis)
    return swaps(lambda s: take(tiles, me ^ s), axis)


def gathered(value, axis):
    return swaps(lambda s: value, axis)


def summed(parts):
    parts = [p.astype(FULL) for p in parts]
    return (parts[0] + parts[1]) + (parts[2] + parts[3])


def everyone(value):
    copies = jnp.broadcast_to(value, (8, *value.shape))
    return lax.all_to_all(copies, ROW, 0, 0, tiled=True)


def dot(a, b):
    return jnp.dot(a, b, preferred_element_type=FULL)


def dot_t(a, b):
    return lax.dot_general(a, b, (((1,), (1,)), ((), ())), preferred_element_type=FULL)


def rounded(value):
    return lax.reduce_precision(value, 8, 7)


def prepare_body(start_ref, support_ref, measured_ref, matrix_ref, kept_ref, slope_ref, index_ref, total):
    tile = pl.program_id(0)
    start = start_ref[0]
    columns = TILE * pl.num_programs(0)
    length = support_ref.shape[1]

    @pl.when(tile == 0)
    def _():
        total[...] = jnp.zeros_like(total)
        lane = lax.broadcasted_iota(jnp.int32, (1, KMAX), 1)
        index_ref[...] = jnp.full(index_ref.shape, -1, jnp.int32)
        for t in range(STEPS + 1):
            row = support_ref[t : t + 1, :]
            below = jnp.sum((row < start).astype(FULL)).astype(jnp.int32)
            until = jnp.sum((row < start + columns).astype(FULL)).astype(jnp.int32)
            first = jnp.minimum((below // KMAX) * KMAX, length - 2 * KMAX)
            near = support_ref[:, pl.ds(pl.multiple_of(first, KMAX), 2 * KMAX)][t : t + 1, :]
            near = jnp.broadcast_to(near, (8, 2 * KMAX))
            shift = (2 * KMAX - (below - first)) & (2 * KMAX - 1)
            near = pltpu.roll(near, shift, 1)[:1, :KMAX] - start
            index_ref[t : t + 1, :] = jnp.where(lane < until - below, near, -1)

    picked = jnp.concatenate([index_ref[t : t + 1, :] for t in range(STEPS)], axis=1)
    place = lax.broadcasted_iota(jnp.int32, (TILE, STEPS * KMAX), 0) + tile * TILE
    chosen = jnp.where(place == picked, 1.0, 0.0).astype(HALF)
    total[...] += dot(matrix_ref[...], chosen)

    @pl.when(tile == pl.num_programs(0) - 1)
    def _():
        slope_ref[...] = dot(
            measured_ref[...].astype(HALF), total[:, :KMAX].astype(HALF)
        ).astype(HALF)
        kept_ref[: STEPS * KMAX, :] = total[...].T.astype(HALF)
        index = jnp.concatenate([index_ref[...]] * 2, axis=0)
        codes = jnp.concatenate([(index >> 6).astype(FULL), (index & 63).astype(FULL)], axis=1)
        rest = jnp.zeros((16, kept_ref.shape[1] - 2 * KMAX), FULL)
        kept_ref[STEPS * KMAX :, :] = jnp.concatenate([codes, rest], axis=1).astype(HALF)


def prepare(start, support, measured, matrix):
    signals, rows = measured.shape
    columns = matrix.shape[1]
    return pl.pallas_call(
        prepare_body,
        grid=(columns // TILE,),
        in_specs=[
            pl.BlockSpec(memory_space=pltpu.SMEM),
            pl.BlockSpec(support.shape, lambda k: (0, 0)),
            pl.BlockSpec(measured.shape, lambda k: (0, 0)),
            pl.BlockSpec((rows, TILE), lambda k: (0, k)),
        ],
        out_specs=[
            pl.BlockSpec((STEPS * KMAX + 16, rows), lambda k: (0, 0)),
            pl.BlockSpec((signals, KMAX), lambda k: (0, 0)),
            pl.BlockSpec((8, KMAX), lambda k: (0, 0)),
        ],
        out_shape=[
            jax.ShapeDtypeStruct((STEPS * KMAX + 16, rows), HALF),
            jax.ShapeDtypeStruct((signals, KMAX), HALF),
            jax.ShapeDtypeStruct((8, KMAX), jnp.int32),
        ],
        scratch_shapes=[pltpu.VMEM((rows, STEPS * KMAX), FULL)],
        cost_estimate=pl.CostEstimate(
            flops=2 * rows * columns * STEPS * KMAX, bytes_accessed=2 * rows * columns, transcendentals=0
        ),
    )(start[None], support, measured, matrix)


def local(matrix, measured, support):
    signals, rows = measured.shape
    columns = matrix.shape[1]
    zl, x, y, zh, c = (lax.axis_index(a) for a in (*ROW, *COL))
    few = signals // 8
    wide = 8 * KMAX
    kept, slope, index = prepare(((y * 4 + zh) * 2 + c) * columns, support, measured, matrix)

    mine = jnp.stack(spread(slope.reshape(4, 2 * few, KMAX), "y")).reshape(4, 2, few, KMAX)
    mine = jnp.moveaxis(mine, 1, 0)
    pair = jnp.stack([take(mine, c), swap(take(mine, 1 - c), "c", 1)])
    partial = jnp.transpose(pair.reshape(8, few, KMAX), (1, 0, 2)).reshape(few, wide)

    near = jnp.stack(gathered(kept, "y"))
    far = swap(near, "c", 1)
    bases = [
        jnp.concatenate([p[:, t * KMAX : (t + 1) * KMAX] for p in (near, far)]).reshape(wide, rows)
        for t in range(STEPS)
    ]
    codes = jnp.concatenate([p[:, STEPS * KMAX :] for p in (near, far)]).astype(FULL)
    codes = codes[:, :, :KMAX] * 64 + codes[:, :, KMAX : 2 * KMAX]

    target = take(measured.reshape(8, few, rows), y * 2 + c)

    def carry(current, t):
        same = (codes[:, t - 1, :, None] == codes[:, t, None, :]) & (codes[:, t - 1, :, None] >= 0)
        high = rounded(current)
        low = current - high
        values = jnp.concatenate([high, low]).astype(HALF).reshape(2 * few, 8, KMAX)
        moved = lax.dot_general(
            values, same.astype(HALF), (((2,), (1,)), ((1,), (0,))), preferred_element_type=FULL
        )
        moved = jnp.transpose(moved[:, :few] + moved[:, few:], (1, 0, 2))
        return moved.reshape(few, wide)

    def energy_of(residual):
        return jnp.sum((residual * residual).reshape(few, rows // KMAX, KMAX), axis=(0, 1))

    copies = jnp.broadcast_to(partial, (8, few, wide))
    current = None
    residual = target
    energies = [energy_of(residual)]
    for t in range(STEPS):
        gradient = lax.all_to_all(copies, ROW, 0, 0, tiled=True).astype(FULL).sum(axis=0)
        stepped = STEP_SIZE * gradient
        current = stepped if t == 0 else carry(current, t) + stepped
        image = dot(current.astype(HALF), bases[t]).astype(HALF)
        residual = target - summed(gathered(image, "zh"))
        if t + 1 < STEPS:
            repeated = jnp.broadcast_to(residual.astype(HALF), (8, few, rows)).reshape(signals, rows)
            copies = dot_t(repeated, bases[t + 1]).astype(HALF).reshape(8, few, wide)
        energies.append(energy_of(lax.optimization_barrier(residual)))

    notes = jnp.stack(energies)
    high = rounded(notes)
    middle = rounded(notes - high)
    notes = jnp.concatenate([high, middle, notes - high - middle])
    notes = jnp.pad(notes, ((0, few - 12), (0, 0))).astype(HALF)
    residual = residual.astype(HALF)
    blocks = current.astype(HALF)
    one = jnp.concatenate([residual, notes, blocks[:, : wide // 2]], axis=1)
    other = swap(jnp.concatenate([residual, notes, blocks[:, wide // 2 :]], axis=1), "c", 1)
    both = jnp.concatenate([jnp.where(c == 0, one, other), jnp.where(c == 0, other, one)])
    fixed = both[:, : rows + KMAX]
    ours = [both[:, rows + (1 + s) * KMAX : rows + (2 + s) * KMAX] for s in range(4)]
    arrived = jnp.stack(
        swaps(lambda s: jnp.concatenate([fixed, ours[s]], axis=1), "y")
    ).reshape(8, few, rows + 2 * KMAX)

    def block(sx, sz):
        number = (zl ^ sz) * 4 + (x ^ sx)
        return take(arrived, (number >> 1 ^ y) * 2 + (number & 1))

    x_major = jnp.concatenate([block(sx, sz)[:, :rows] for sx in range(4) for sz in range(2)])
    z_major = jnp.concatenate([block(sx, sz)[:, :rows] for sz in range(2) for sx in range(4)])
    half = columns // 2
    left = dot(x_major, matrix[:, :half]).astype(HALF).reshape(4, 2 * few, half)
    right = dot(z_major, matrix[:, half:]).astype(HALF).reshape(2, 4 * few, half)
    crossed = swap(right[1], "zl", 1)
    left = summed(swaps(lambda s: left[s], "x"))
    right = (right[0].astype(FULL) + crossed.astype(FULL)).reshape(4, few, half)
    crossed = swap(left[few:].astype(HALF), "zl", 1)
    right = summed(swaps(lambda s: right[s] if s == 0 else right[s].astype(HALF), "x"))
    gradient = jnp.concatenate([left[:few] + crossed.astype(FULL), right], axis=1)

    home = block(0, 0)[:, rows + KMAX :]
    place = jnp.arange(columns)[:, None]
    stepped = dot_t(home, (place == index[2][None, :]).astype(HALF)) + STEP_SIZE * gradient
    keep = jnp.any(index[3][:, None] == jnp.arange(columns)[None, :], axis=0)
    estimate = jnp.where(keep[None, :], stepped, 0.0)

    squares = jnp.sum(stepped * stepped, axis=0).reshape(columns // KMAX, KMAX)
    notes = jnp.sum(arrived[:, :, rows : rows + KMAX].astype(FULL), axis=0)
    totals = jnp.sum(everyone(jnp.concatenate([squares, notes[:16]])), axis=0)
    lines = columns // KMAX
    energy = totals[lines : lines + 12].reshape(3, 4, KMAX).sum(axis=(0, 2))
    return (
        estimate,
        jnp.sqrt(totals[:lines]).reshape(columns),
        energy / (signals * rows * 8),
    )


def solution(mesh):
    torus = Mesh(mesh.devices.reshape(2, 4, 4, 4, 2), (*ROW, *COL))
    return jax.shard_map(
        local,
        mesh=torus,
        in_specs=(P(ROW, COL), P(None, ROW), P()),
        out_specs=(P(ROW, COL), P(COL), P()),
        check_vma=False,
    )
```
